32 devices in a mesh: ep: 32 (over z, y, x, core).
Axes of the slice: x: 2, y: 2, z: 4, core: 2. Of those that a mesh axis runs over, the one named last changes fastest.
Arguments:
- hidden: bfloat16 [65536, 1024], P('ep')
- w_router: float32 [1024, 32], replicated
- expert_ids: int32 [65536, 2], P('ep')
- w_one: bfloat16 [32, 1024, 2816], P('ep')
- w_three: bfloat16 [32, 1024, 2816], P('ep')
- w_two: bfloat16 [32, 2816, 1024], P('ep')
Outputs:
- output: bfloat16 [65536, 1024], P('ep')
All inputs are finite; a program needn't handle non-finite values.
Results may differ from the reference program's by a relative error of at most 0.00868986.
Values are sent between devices in bfloat16 or wider.
A program may use at most 1 GiB of HBM per device.

```python
import jax
import jax.numpy as jnp
from jax import lax

TOK_DEV = 2048
GROUP = 32
D = 1024
FF = 2816
EXPERTS = 32
ROW_BLOCK = 32


def route_ids(key):
    key_hot, key_src = jax.random.split(key)
    dev_order = jax.random.permutation(key_hot, GROUP)
    n_hot = GROUP // 4
    n_cold = GROUP - n_hot
    row_cap = 4 * TOK_DEV // GROUP
    per_dev = EXPERTS // GROUP
    hot_devs = dev_order[:n_hot]
    cold_devs = dev_order[n_hot:]
    slot_idx = jnp.arange(TOK_DEV)

    def one_source(src_key):
        key_shift, key_first, key_second, key_flip, key_perm = jax.random.split(src_key, 5)
        shift_val = jax.random.randint(key_shift, (), 0, n_cold)
        first_dev = hot_devs[slot_idx // row_cap]
        second_dev = cold_devs[(slot_idx + shift_val) % n_cold]
        first_exp = first_dev * per_dev + jax.random.randint(key_first, (TOK_DEV,), 0, per_dev)
        second_exp = second_dev * per_dev + jax.random.randint(key_second, (TOK_DEV,), 0, per_dev)
        pair_ids = jnp.stack([first_exp, second_exp], axis=1)
        flip_bit = jax.random.randint(key_flip, (TOK_DEV, 1), 0, 2)
        pair_ids = jnp.where(flip_bit == 1, pair_ids[:, ::-1], pair_ids)
        token_perm = jax.random.permutation(key_perm, TOK_DEV)
        return pair_ids[token_perm]

    src_keys = jax.random.split(key_src, GROUP)
    return jax.vmap(one_source)(src_keys).reshape(GROUP * TOK_DEV, 2).astype(jnp.int32)


def setup_inputs(seed: int = 0) -> dict:
    key = jax.random.key(seed)
    key_hidden, key_router, key_ids, key_one, key_three, key_two = jax.random.split(key, 6)
    tok_count = GROUP * TOK_DEV
    hidden = jax.random.normal(key_hidden, (tok_count, D), jnp.float32).astype(jnp.bfloat16)
    w_router = jax.random.normal(key_router, (D, EXPERTS), jnp.float32) * D ** -0.5
    expert_ids = route_ids(key_ids)
    w_one = (jax.random.normal(key_one, (EXPERTS, D, FF), jnp.float32) * D ** -0.5).astype(jnp.bfloat16)
    w_three = (jax.random.normal(key_three, (EXPERTS, D, FF), jnp.float32) * D ** -0.5).astype(jnp.bfloat16)
    w_two = (jax.random.normal(key_two, (EXPERTS, FF, D), jnp.float32) * FF ** -0.5).astype(jnp.bfloat16)
    return {"hidden": hidden, "w_router": w_router, "expert_ids": expert_ids, "w_one": w_one, "w_three": w_three, "w_two": w_two}


def reference(hidden, w_router, expert_ids, w_one, w_three, w_two):
    tok_count = hidden.shape[0]
    model_dim = hidden.shape[1]
    logits = jnp.dot(hidden.astype(jnp.float32), w_router, preferred_element_type=jnp.float32)
    prob_vals = jax.nn.softmax(logits, axis=-1)
    picked = jnp.take_along_axis(prob_vals, expert_ids, axis=1)
    gate_vals = picked / jnp.sum(picked, axis=1, keepdims=True)
    flat_ids = expert_ids.reshape(-1)
    assign_count = flat_ids.shape[0]
    sort_order = jnp.argsort(flat_ids, stable=True)
    sorted_ids = flat_ids[sort_order]
    counts = jnp.zeros((EXPERTS,), jnp.int32).at[flat_ids].add(1)
    padded = (counts + ROW_BLOCK - 1) // ROW_BLOCK * ROW_BLOCK
    pad_end = jnp.cumsum(padded)
    pad_start = pad_end - padded
    first_row = jnp.cumsum(counts) - counts
    rank_in = jnp.arange(assign_count) - first_row[sorted_ids]
    dest_row = pad_start[sorted_ids] + rank_in
    row_total = assign_count + EXPERTS * ROW_BLOCK
    block_count = row_total // ROW_BLOCK
    row_tok = jnp.zeros((row_total,), jnp.int32).at[dest_row].set((sort_order // 2).astype(jnp.int32))
    block_start = jnp.arange(block_count) * ROW_BLOCK
    block_exp = jnp.minimum(jnp.sum((block_start[:, None] >= pad_end[None, :]).astype(jnp.int32), axis=1), EXPERTS - 1)
    hidden_blocks = hidden[row_tok].reshape(block_count, ROW_BLOCK, model_dim)

    def block_ffn(block_args):
        hid_blk, exp_idx = block_args
        h_one = jnp.dot(hid_blk, w_one[exp_idx], preferred_element_type=jnp.float32)
        h_three = jnp.dot(hid_blk, w_three[exp_idx], preferred_element_type=jnp.float32)
        act_rows = (jax.nn.silu(h_one) * h_three).astype(jnp.bfloat16)
        return jnp.dot(act_rows, w_two[exp_idx], preferred_element_type=jnp.float32).astype(jnp.bfloat16)

    out_blocks = lax.map(block_ffn, (hidden_blocks, block_exp))
    out_rows = out_blocks.reshape(row_total, model_dim)
    sorted_out = out_rows[dest_row]
    assign_out = jnp.zeros((assign_count, model_dim), jnp.bfloat16).at[sort_order].set(sorted_out)
    both_out = assign_out.reshape(tok_count, 2, model_dim).astype(jnp.float32)
    out_sum = jnp.sum(gate_vals[:, :, None] * both_out, axis=1)
    return out_sum.astype(jnp.bfloat16)
```

```python
import functools

import jax
import jax.numpy as jnp
from jax import lax
from jax.experimental import pallas as pl
from jax.experimental.pallas import tpu as pltpu
from jax.sharding import PartitionSpec as P

MESH = pl.DeviceIdType.MESH
NZ = 4
NQ = 8
HALVES = 2


def moe_kernel(hid_hbm, ids_ref, w1_hbm, w3_hbm, w2_hbm, back_hbm, pos_ref,
               hid, send, recv, w1, w3, w2, act, sel, rank, rank_in,
               own_sem, w_sem, z_send, z_recv, r_send, r_recv,
               p_send, p_recv, b_send, b_recv, loc_sem):
    me = lax.axis_index("ep")
    z = me // NQ
    q = me % NQ
    mirror = z // 2
    zz = z + mirror * (3 - 2 * z)
    tok = hid_hbm.shape[0]
    dim = hid_hbm.shape[1]
    ff = w1.shape[1]
    cap = back_hbm.shape[1]
    half_tok = tok // HALVES
    pair = 2 * cap
    nt = min(256, dim)
    ft = min(256, ff)

    def block_of(step):
        near = (0, 1, 2, 3)[step]
        inner = (1, 2, 0, 3)[step]
        pick = near + zz * (inner - near)
        return pick + mirror * (3 - 2 * pick)

    def half(ref, h):
        return ref.at[pl.ds(h * half_tok, half_tok)]

    def z_copy(direction, hop, h, block, src=None):
        target = me + (NQ if direction == 0 else -NQ)
        return pltpu.make_async_remote_copy(
            src_ref=half(hid.at[block] if src is None else src, h),
            dst_ref=half(hid.at[block], h),
            send_sem=z_send.at[direction, hop - 1, h],
            recv_sem=z_recv.at[direction, hop - 1, h],
            device_id=(target,), device_id_type=MESH)

    def rank_copy(plane):
        return pltpu.make_async_remote_copy(
            src_ref=rank.at[plane], dst_ref=rank_in.at[z],
            send_sem=r_send.at[plane], recv_sem=r_recv.at[z],
            device_id=(plane * NQ + q,), device_id_type=MESH)

    def plane_copy(step, peer):
        return pltpu.make_async_remote_copy(
            src_ref=send.at[pl.ds(peer * cap, cap)],
            dst_ref=recv.at[step, pl.ds(q * cap, cap)],
            send_sem=p_send.at[peer], recv_sem=p_recv.at[step, q],
            device_id=(z * NQ + peer,), device_id_type=MESH)

    def plane_arrival(step, peer):
        return pltpu.make_async_remote_copy(
            src_ref=send.at[pl.ds(peer * cap, cap)],
            dst_ref=recv.at[step, pl.ds(peer * cap, cap)],
            send_sem=p_send.at[peer], recv_sem=p_recv.at[step, peer],
            device_id=(z * NQ + peer,), device_id_type=MESH)

    def back_copy(step, peer):
        return pltpu.make_async_remote_copy(
            src_ref=recv.at[step, pl.ds(peer * cap, cap)],
            dst_ref=back_hbm.at[me],
            send_sem=b_send.at[step, peer], recv_sem=b_recv.at[me],
            device_id=(block_of(step) * NQ + peer,), device_id_type=MESH)

    own_load = pltpu.make_async_copy(hid_hbm, hid.at[z], own_sem)
    for h in range(HALVES):
        @pl.when(z < NZ - 1)
        def _():
            z_copy(0, 1, h, z, hid_hbm).start()

        @pl.when(z > 0)
        def _():
            z_copy(1, 1, h, z, hid_hbm).start()
    own_load.start()
    w_loads = [pltpu.make_async_copy(src, dst, w_sem.at[k])
               for k, (src, dst) in enumerate(((w1_hbm, w1), (w3_hbm, w3), (w2_hbm, w2)))]
    for load in w_loads:
        load.start()

    n_exp = NZ * NQ
    lanes = min(256, tok)
    exp_iota = lax.broadcasted_iota(jnp.int32, (n_exp, lanes), 0)
    row_iota = lax.broadcasted_iota(jnp.int32, (lanes, lanes), 0)
    col_iota = lax.broadcasted_iota(jnp.int32, (lanes, lanes), 1)
    below = (row_iota < col_iota).astype(jnp.float32).astype(jnp.bfloat16)
    carry = jnp.zeros((n_exp, 1), jnp.float32)
    for k in range(tok // lanes):
        span = pl.ds(k * lanes, lanes)
        first = ids_ref[pl.ds(0, 1), span] == exp_iota
        second = ids_ref[pl.ds(1, 1), span] == exp_iota
        chosen = jnp.where(first, 1.0, 0.0) + jnp.where(second, 1.0, 0.0)
        count = jnp.dot(chosen.astype(jnp.bfloat16), below, preferred_element_type=jnp.float32) + carry
        carry = carry + jnp.sum(chosen, axis=1, keepdims=True)
        marked = jnp.where(chosen > 0.5, count, -1.0)
        for plane in range(NZ):
            rank[plane, :, span] = marked[plane * NQ:(plane + 1) * NQ]
        slot0 = jnp.sum(jnp.where(first, count, 0.0), axis=0, keepdims=True).astype(jnp.int32)
        slot1 = jnp.sum(jnp.where(second, count, 0.0), axis=0, keepdims=True).astype(jnp.int32)
        pos_ref[pl.ds(0, 1), span] = ids_ref[pl.ds(0, 1), span] * cap + slot0
        pos_ref[pl.ds(1, 1), span] = ids_ref[pl.ds(1, 1), span] * cap + slot1
    for plane in range(NZ):
        @pl.when(z != plane)
        def _():
            rank_copy(plane).start()

        @pl.when(z == plane)
        def _():
            rank_in[plane] = rank[plane]

    def relay(hop, h):
        @pl.when(z >= hop)
        def _():
            z_copy(0, hop, h, z - hop).wait_recv()

        @pl.when(jnp.logical_and(z >= hop, z < NZ - 1))
        def _():
            z_copy(0, hop + 1, h, z - hop).start()

        @pl.when(z + hop < NZ)
        def _():
            z_copy(1, hop, h, z + hop).wait_recv()

        @pl.when(jnp.logical_and(z + hop < NZ, z > 0))
        def _():
            z_copy(1, hop + 1, h, z + hop).start()

    def select(step):
        block = block_of(step)
        if step > 0:
            pltpu.make_async_remote_copy(
                src_ref=rank.at[0], dst_ref=rank_in.at[block],
                send_sem=r_send.at[block], recv_sem=r_recv.at[block],
                device_id=(block * NQ + q,), device_id_type=MESH).wait_recv()
        slot_iota = lax.broadcasted_iota(jnp.int32, (cap, tok), 0).astype(jnp.float32)

        @pl.loop(0, NQ // 2)
        def _(k):
            p = (q // 2 + 1 + k) % (NQ // 2)
            for j in range(2):
                peer = 2 * p + j
                if step > 0:
                    @pl.when(peer != q)
                    def _():
                        plane_copy(step - 1, peer).wait_send()
                row = rank_in[block, pl.ds(peer, 1), :]
                sel[pl.ds(j * cap, cap), :] = jnp.where(slot_iota == row, 1.0, 0.0).astype(jnp.bfloat16)

            @pl.loop(0, dim // nt)
            def _(n):
                cols = pl.ds(pl.multiple_of(n * nt, nt), nt)
                send[pl.ds(p * pair, pair), cols] = jnp.dot(
                    sel[...], hid[block, :, cols], preferred_element_type=jnp.float32).astype(jnp.bfloat16)

            for j in range(2):
                peer = 2 * p + j

                @pl.when(peer != q)
                def _():
                    plane_copy(step, peer).start()

                @pl.when(peer == q)
                def _():
                    recv[step, pl.ds(peer * cap, cap), :] = send[pl.ds(peer * cap, cap), :]

    def experts(step):
        block = block_of(step)

        @pl.loop(0, NQ // 2)
        def _(k):
            p = (q // 2 + NQ // 2 - k) % (NQ // 2)
            for j in range(2):
                peer = 2 * p + j

                @pl.when(peer != q)
                def _():
                    plane_arrival(step, peer).wait_recv()
            rows = pl.ds(p * pair, pair)

            @pl.loop(0, ff // ft)
            def _(f):
                cols = pl.ds(pl.multiple_of(f * ft, ft), ft)
                x = recv[step, rows, :]
                u = jnp.dot(x, w1[:, cols], preferred_element_type=jnp.float32)
                v = jnp.dot(x, w3[:, cols], preferred_element_type=jnp.float32)
                act[:, cols] = (jax.nn.silu(u) * v).astype(jnp.bfloat16)

            @pl.loop(0, dim // nt)
            def _(n):
                cols = pl.ds(pl.multiple_of(n * nt, nt), nt)
                recv[step, rows, cols] = jnp.dot(
                    act[...], w2[:, cols], preferred_element_type=jnp.float32).astype(jnp.bfloat16)

            for j in range(2):
                peer = 2 * p + j
                home = block * NQ + peer

                @pl.when(home != me)
                def _():
                    back_copy(step, peer).start()

                @pl.when(home == me)
                def _():
                    pltpu.make_async_copy(recv.at[step, pl.ds(peer * cap, cap)], back_hbm.at[me], loc_sem).start()

    own_load.wait()
    select(0)
    relay(1, 0)
    relay(1, 1)
    select(1)
    for load in w_loads:
        load.wait()
    experts(0)
    relay(2, 0)

    @pl.when(zz == 0)
    def _():
        relay(2, 1)
    select(2)
    experts(1)

    @pl.when(zz == 1)
    def _():
        relay(2, 1)
    for h in range(HALVES):
        @pl.when(z >= 3)
        def _():
            z_copy(0, 3, h, z - 3).wait_recv()

        @pl.when(z + 3 < NZ)
        def _():
            z_copy(1, 3, h, z + 3).wait_recv()
    select(3)
    experts(2)
    experts(3)

    for h in range(HALVES):
        for hop in range(1, NZ):
            @pl.when(jnp.logical_and(z < NZ - 1, z >= hop - 1))
            def _():
                z_copy(0, hop, h, z - (hop - 1)).wait_send()

            @pl.when(jnp.logical_and(z > 0, z + (hop - 1) < NZ))
            def _():
                z_copy(1, hop, h, z + (hop - 1)).wait_send()
    for plane in range(NZ):
        @pl.when(z != plane)
        def _():
            rank_copy(plane).wait_send()

    @pl.loop(0, NQ)
    def _(peer):
        @pl.when(peer != q)
        def _():
            plane_copy(NZ - 1, peer).wait_send()
        for step in range(NZ):
            @pl.when(block_of(step) * NQ + peer != me)
            def _():
                back_copy(step, peer).wait_send()
    pltpu.make_async_copy(recv.at[0, pl.ds(q * cap, cap)], back_hbm.at[me], loc_sem).wait()

    @pl.loop(1, NZ * NQ)
    def _(k):
        other = (me + k) % (NZ * NQ)
        pltpu.make_async_remote_copy(
            src_ref=recv.at[0, pl.ds(0, cap)], dst_ref=back_hbm.at[other],
            send_sem=b_send.at[0, 0], recv_sem=b_recv.at[other],
            device_id=(other,), device_id_type=MESH).wait_recv()


def moe_exchange(hidden_loc, ids_t, w_one, w_three, w_two, n):
    tok, dim = hidden_loc.shape
    ff = w_one.shape[1]
    cap = 4 * tok // n
    any_spec = pl.BlockSpec(memory_space=pl.ANY)
    vmem_spec = pl.BlockSpec(memory_space=pltpu.VMEM)
    dma = pltpu.SemaphoreType.DMA
    rows = n * cap
    flops = 2 * rows * (3 * dim * ff + tok * dim)
    return pl.pallas_call(
        moe_kernel,
        out_shape=(jax.ShapeDtypeStruct((n, cap, dim), jnp.bfloat16),
                   jax.ShapeDtypeStruct((2, tok), jnp.int32)),
        in_specs=[any_spec, vmem_spec, any_spec, any_spec, any_spec],
        out_specs=(any_spec, vmem_spec),
        scratch_shapes=[
            pltpu.VMEM((NZ, tok, dim), jnp.bfloat16),
            pltpu.VMEM((NQ * cap, dim), jnp.bfloat16),
            pltpu.VMEM((NZ, NQ * cap, dim), jnp.bfloat16),
            pltpu.VMEM((dim, ff), jnp.bfloat16),
            pltpu.VMEM((dim, ff), jnp.bfloat16),
            pltpu.VMEM((ff, dim), jnp.bfloat16),
            pltpu.VMEM((2 * cap, ff), jnp.bfloat16),
            pltpu.VMEM((2 * cap, tok), jnp.bfloat16),
            pltpu.VMEM((NZ, NQ, tok), jnp.float32),
            pltpu.VMEM((NZ, NQ, tok), jnp.float32),
            dma(()), dma((3,)), dma((2, NZ - 1, HALVES)), dma((2, NZ - 1, HALVES)),
            dma((NZ,)), dma((NZ,)), dma((NQ,)), dma((NZ, NQ)),
            dma((NZ, NQ)), dma((NZ * NQ,)), dma(()),
        ],
        compiler_params=pltpu.CompilerParams(has_side_effects=True, vmem_limit_bytes=67043328),
        cost_estimate=pl.CostEstimate(flops=flops, bytes_accessed=2 * rows * dim * 4, transcendentals=rows * ff),
    )(hidden_loc, ids_t, w_one, w_three, w_two)


def route_gates(hidden_loc, w_router, ids_loc):
    logits = jnp.dot(hidden_loc.astype(jnp.float32), w_router, preferred_element_type=jnp.float32)
    prob_vals = jax.nn.softmax(logits, axis=-1)
    exp_iota = lax.broadcasted_iota(jnp.int32, prob_vals.shape, 1)
    p_a = jnp.sum(jnp.where(exp_iota == ids_loc[:, 0:1], prob_vals, 0.0), axis=1, keepdims=True)
    p_b = jnp.sum(jnp.where(exp_iota == ids_loc[:, 1:2], prob_vals, 0.0), axis=1, keepdims=True)
    total = p_a + p_b
    return p_a / total, p_b / total


def solution(mesh):
    n = mesh.shape["ep"]

    def device_body(hidden_loc, w_router, ids_loc, w_one, w_three, w_two):
        dim = hidden_loc.shape[1]
        back, pos = moe_exchange(hidden_loc, ids_loc.T, w_one[0], w_three[0], w_two[0], n)
        flat = back.reshape(-1, dim)
        g_a, g_b = route_gates(hidden_loc, w_router, ids_loc)
        e_a = jnp.take(flat, pos[0], axis=0, mode="clip").astype(jnp.float32)
        e_b = jnp.take(flat, pos[1], axis=0, mode="clip").astype(jnp.float32)
        return (g_a * e_a + g_b * e_b).astype(jnp.bfloat16)

    return jax.shard_map(device_body, mesh=mesh, in_specs=(P("ep", None), P(None, None), P("ep", None), P("ep", None, None), P("ep", None, None), P("ep", None, None)), out_specs=P("ep", None), check_vma=False)
```

```python
import functools

import jax
import jax.numpy as jnp
from jax import lax
from jax.experimental import pallas as pl
from jax.experimental.pallas import tpu as pltpu
from jax.sharding import PartitionSpec as P

MESH = pl.DeviceIdType.MESH
NZ = 4
NQ = 8
HALVES = 2
PIECES = 4


def moe_kernel(limit, cap, hid_hbm, ids_ref, w1_hbm, w3_hbm, w2_hbm, rows_hbm, land_hbm, pos_ref,
               hid, send, recv, w1, w3, w2, act, sel, rank, rank_in, slots,
               own_sem, w_sem, z_send, z_recv, r_send, r_recv,
               p_send, p_recv, l_send, l_recv, loc_sem, stage_sem, b_send, b_recv):
    me = lax.axis_index("ep")
    z = me // NQ
    q = me % NQ
    mirror = z // 2
    zz = z + mirror * (3 - 2 * z)
    tok = hid_hbm.shape[0]
    dim = hid_hbm.shape[1]
    ff = w1.shape[1]
    piece = limit // PIECES
    back_base = NQ * cap
    half_tok = tok // HALVES
    pair = 2 * cap
    nt = min(256, dim)
    ft = min(256, ff)

    def block_of(step):
        near = (0, 1, 2, 3)[step]
        inner = (1, 2, 3, 0)[step]
        pick = near + zz * (inner - near)
        return pick + mirror * (3 - 2 * pick)

    def partner(c):
        px, py = (q // 2) % 2, q // 4
        return 2 * (py + (c // 2) * (1 - 2 * py)) + px + (c % 2) * (1 - 2 * px)

    def half(ref, h):
        return ref.at[pl.ds(h * half_tok, half_tok)]

    def z_copy(direction, hop, h, block, src=None):
        target = me + (NQ if direction == 0 else -NQ)
        return pltpu.make_async_remote_copy(
            src_ref=half(hid.at[block] if src is None else src, h),
            dst_ref=half(hid.at[block], h),
            send_sem=z_send.at[direction, hop - 1, h],
            recv_sem=z_recv.at[direction, hop - 1, h],
            device_id=(target,), device_id_type=MESH)

    def rank_copy(plane):
        return pltpu.make_async_remote_copy(
            src_ref=rank.at[plane], dst_ref=rank_in.at[z],
            send_sem=r_send.at[plane], recv_sem=r_recv.at[z],
            device_id=(plane * NQ + q,), device_id_type=MESH)

    def plane_copy(step, peer):
        return pltpu.make_async_remote_copy(
            src_ref=send.at[pl.ds(peer * cap, cap)],
            dst_ref=recv.at[step, pl.ds(q * cap, cap)],
            send_sem=p_send.at[peer], recv_sem=p_recv.at[step, q],
            device_id=(z * NQ + peer,), device_id_type=MESH)

    def plane_arrival(step, peer):
        return pltpu.make_async_remote_copy(
            src_ref=send.at[pl.ds(peer * cap, cap)],
            dst_ref=recv.at[step, pl.ds(peer * cap, cap)],
            send_sem=p_send.at[peer], recv_sem=p_recv.at[step, peer],
            device_id=(z * NQ + peer,), device_id_type=MESH)

    def landing(step, peer):
        home = rows_hbm if step == 0 else land_hbm.at[step - 1]
        return home.at[pl.ds(peer * cap, cap)]

    def land_copy(step, peer):
        return pltpu.make_async_remote_copy(
            src_ref=recv.at[step, pl.ds(peer * cap, cap)], dst_ref=landing(step, q),
            send_sem=l_send.at[step, peer], recv_sem=l_recv.at[step, q],
            device_id=(z * NQ + peer,), device_id_type=MESH)

    def land_arrival(step, peer):
        return pltpu.make_async_remote_copy(
            src_ref=recv.at[step, pl.ds(peer * cap, cap)], dst_ref=landing(step, peer),
            send_sem=l_send.at[step, peer], recv_sem=l_recv.at[step, peer],
            device_id=(z * NQ + peer,), device_id_type=MESH)

    def land_own(step):
        return pltpu.make_async_copy(recv.at[step, pl.ds(q * cap, cap)], landing(step, q), loc_sem.at[step])

    def back_copy(step, g, plane, owner):
        return pltpu.make_async_remote_copy(
            src_ref=recv.at[step, pl.ds(g * piece, piece)],
            dst_ref=rows_hbm.at[pl.ds(back_base + plane * limit + g * piece, piece)],
            send_sem=b_send.at[step, g], recv_sem=b_recv.at[plane, g],
            device_id=(owner * NQ + q,), device_id_type=MESH)

    own_load = pltpu.make_async_copy(hid_hbm, hid.at[z], own_sem)
    for h in range(HALVES):
        @pl.when(z < NZ - 1)
        def _():
            z_copy(0, 1, h, z, hid_hbm).start()

        @pl.when(z > 0)
        def _():
            z_copy(1, 1, h, z, hid_hbm).start()
    own_load.start()
    w_loads = [pltpu.make_async_copy(src, dst, w_sem.at[k])
               for k, (src, dst) in enumerate(((w1_hbm, w1), (w3_hbm, w3), (w2_hbm, w2)))]
    for load in w_loads:
        load.start()

    n_exp = NZ * NQ
    lanes = min(256, tok)
    exp_iota = lax.broadcasted_iota(jnp.int32, (n_exp, lanes), 0)
    row_iota = lax.broadcasted_iota(jnp.int32, (lanes, lanes), 0)
    col_iota = lax.broadcasted_iota(jnp.int32, (lanes, lanes), 1)
    below = (row_iota < col_iota).astype(jnp.float32).astype(jnp.bfloat16)
    carry = jnp.zeros((n_exp, 1), jnp.float32)
    for k in range(tok // lanes):
        span = pl.ds(k * lanes, lanes)
        first = ids_ref[pl.ds(0, 1), span] == exp_iota
        second = ids_ref[pl.ds(1, 1), span] == exp_iota
        chosen = jnp.where(first, 1.0, 0.0) + jnp.where(second, 1.0, 0.0)
        count = jnp.dot(chosen.astype(jnp.bfloat16), below, preferred_element_type=jnp.float32) + carry
        carry = carry + jnp.sum(chosen, axis=1, keepdims=True)
        marked = jnp.where(chosen > 0.5, count, -1.0)
        for plane in range(NZ):
            rank[plane, :, span] = marked[plane * NQ:(plane + 1) * NQ]
    for plane in range(NZ):
        @pl.when(z != plane)
        def _():
            rank_copy(plane).start()

        @pl.when(z == plane)
        def _():
            rank_in[plane] = rank[plane]

    base = []
    for plane in range(NZ):
        run = jnp.zeros((1, 1), jnp.float32)
        for e in range(NQ):
            there = run + (back_base + plane * limit)
            base.append(jnp.where(z == plane, float(e * cap), there))
            run = run + carry[plane * NQ + e:plane * NQ + e + 1, :]
    base = jnp.concatenate(base, axis=0)
    for k in range(tok // lanes):
        span = pl.ds(k * lanes, lanes)
        place = jnp.concatenate([rank[plane, :, span] for plane in range(NZ)], axis=0) + base
        for j in range(2):
            hit = ids_ref[pl.ds(j, 1), span] == exp_iota
            pos_ref[pl.ds(j, 1), span] = jnp.sum(
                jnp.where(hit, place, 0.0), axis=0, keepdims=True).astype(jnp.int32)

    def relay(hop, h):
        @pl.when(z >= hop)
        def _():
            z_copy(0, hop, h, z - hop).wait_recv()

        @pl.when(jnp.logical_and(z >= hop, z < NZ - 1))
        def _():
            z_copy(0, hop + 1, h, z - hop).start()

        @pl.when(z + hop < NZ)
        def _():
            z_copy(1, hop, h, z + hop).wait_recv()

        @pl.when(jnp.logical_and(z + hop < NZ, z > 0))
        def _():
            z_copy(1, hop + 1, h, z + hop).start()

    def select(step):
        block = block_of(step)
        if step > 0:
            pltpu.make_async_remote_copy(
                src_ref=rank.at[0], dst_ref=rank_in.at[block],
                send_sem=r_send.at[block], recv_sem=r_recv.at[block],
                device_id=(block * NQ + q,), device_id_type=MESH).wait_recv()
        slot_iota = lax.broadcasted_iota(jnp.int32, (cap, tok), 0).astype(jnp.float32)

        @pl.loop(0, NQ // 2)
        def _(k):
            p = partner((k + 1) % (NQ // 2))
            for j in range(2):
                peer = 2 * p + j
                if step > 0:
                    @pl.when(peer != q)
                    def _():
                        plane_copy(step - 1, peer).wait_send()
                row = rank_in[block, pl.ds(peer, 1), :]
                sel[pl.ds(j * cap, cap), :] = jnp.where(slot_iota == row, 1.0, 0.0).astype(jnp.bfloat16)

            @pl.loop(0, dim // nt)
            def _(n):
                cols = pl.ds(pl.multiple_of(n * nt, nt), nt)
                send[pl.ds(p * pair, pair), cols] = jnp.dot(
                    sel[...], hid[block, :, cols], preferred_element_type=jnp.float32).astype(jnp.bfloat16)

            for j in range(2):
                peer = 2 * p + j

                @pl.when(peer != q)
                def _():
                    plane_copy(step, peer).start()

                @pl.when(peer == q)
                def _():
                    recv[step, pl.ds(peer * cap, cap), :] = send[pl.ds(peer * cap, cap), :]

    def experts(step):
        @pl.loop(0, NQ // 2)
        def _(k):
            p = partner(k)
            for j in range(2):
                peer = 2 * p + j

                @pl.when(peer != q)
                def _():
                    plane_arrival(step, peer).wait_recv()
            rows = pl.ds(p * pair, pair)

            @pl.loop(0, ff // ft)
            def _(f):
                cols = pl.ds(pl.multiple_of(f * ft, ft), ft)
                x = recv[step, rows, :]
                u = jnp.dot(x, w1[:, cols], preferred_element_type=jnp.float32)
                v = jnp.dot(x, w3[:, cols], preferred_element_type=jnp.float32)
                act[:, cols] = (jax.nn.silu(u) * v).astype(jnp.bfloat16)

            @pl.loop(0, dim // nt)
            def _(n):
                cols = pl.ds(pl.multiple_of(n * nt, nt), nt)
                recv[step, rows, cols] = jnp.dot(
                    act[...], w2[:, cols], preferred_element_type=jnp.float32).astype(jnp.bfloat16)

            for j in range(2):
                peer = 2 * p + j

                @pl.when(peer != q)
                def _():
                    land_copy(step, peer).start()

                @pl.when(peer == q)
                def _():
                    land_own(step).start()

    def landed(step):
        @pl.loop(0, NQ)
        def _(peer):
            @pl.when(peer != q)
            def _():
                land_arrival(step, peer).wait_recv()
                land_copy(step, peer).wait_send()
        land_own(step).wait()

    def give_back(step):
        block = block_of(step)
        for h in range(HALVES):
            @pl.when(jnp.logical_and(block < z, z < NZ - 1))
            def _():
                z_copy(0, z - block + 1, h, block).wait_send()

            @pl.when(jnp.logical_and(block > z, z > 0))
            def _():
                z_copy(1, block - z + 1, h, block).wait_send()
        landed(step)
        stage = pltpu.make_async_copy(land_hbm.at[step - 1], hid.at[block], stage_sem)
        stage.start()
        slot_iota = lax.broadcasted_iota(jnp.int32, (1, cap), 1).astype(jnp.float32)
        run = jnp.zeros((1, 1), jnp.float32)
        for e in range(NQ):
            taken = jnp.sum(jnp.where(rank_in[block, pl.ds(e, 1), :] >= 0.0, 1.0, 0.0), axis=1, keepdims=True)
            slots[pl.ds(e, 1), :] = jnp.where(slot_iota < taken, slot_iota + run, -1.0)
            run = run + taken
        stage.wait()

        @pl.loop(0, PIECES)
        def _(g):
            place = (lax.broadcasted_iota(jnp.int32, (piece, cap), 0) + g * piece).astype(jnp.float32)
            for e in range(NQ):
                sel[pl.ds(0, piece), pl.ds(e * cap, cap)] = jnp.where(
                    place == slots[pl.ds(e, 1), :], 1.0, 0.0).astype(jnp.bfloat16)

            @pl.loop(0, dim // nt)
            def _(n):
                cols = pl.ds(pl.multiple_of(n * nt, nt), nt)
                recv[step, pl.ds(g * piece, piece), cols] = jnp.dot(
                    sel[pl.ds(0, piece), :], hid[block, :, cols],
                    preferred_element_type=jnp.float32).astype(jnp.bfloat16)
            back_copy(step, g, z, block).start()

    own_load.wait()
    select(0)
    relay(1, 0)
    relay(1, 1)
    select(1)
    for load in w_loads:
        load.wait()
    experts(0)
    relay(2, 0)
    experts(1)
    relay(2, 1)
    select(2)
    give_back(1)
    experts(2)
    for h in range(HALVES):
        @pl.when(z >= 3)
        def _():
            z_copy(0, 3, h, z - 3).wait_recv()

        @pl.when(z + 3 < NZ)
        def _():
            z_copy(1, 3, h, z + 3).wait_recv()
    select(3)
    give_back(2)
    experts(3)
    give_back(3)

    for h in range(HALVES):
        @pl.when(z < NZ - 1)
        def _():
            z_copy(0, 1, h, z).wait_send()

        @pl.when(z > 0)
        def _():
            z_copy(1, 1, h, z).wait_send()
    for plane in range(NZ):
        @pl.when(z != plane)
        def _():
            rank_copy(plane).wait_send()

    @pl.loop(0, NQ)
    def _(peer):
        @pl.when(peer != q)
        def _():
            plane_copy(NZ - 1, peer).wait_send()
    landed(0)

    @pl.loop(0, PIECES)
    def _(g):
        for step in range(1, NZ):
            back_copy(step, g, z, block_of(step)).wait_send()
            back_copy(step, g, block_of(step), block_of(step)).wait_recv()


def moe_exchange(hidden_loc, ids_t, w_one, w_three, w_two, n, limit):
    tok, dim = hidden_loc.shape
    ff = w_one.shape[1]
    cap = 4 * tok // n
    any_spec = pl.BlockSpec(memory_space=pl.ANY)
    vmem_spec = pl.BlockSpec(memory_space=pltpu.VMEM)
    dma = pltpu.SemaphoreType.DMA
    rows = n * cap
    flops = 2 * rows * (3 * dim * ff + 2 * tok * dim)
    return pl.pallas_call(
        functools.partial(moe_kernel, limit, cap),
        out_shape=(jax.ShapeDtypeStruct((NQ * cap + NZ * limit, dim), jnp.bfloat16),
                   jax.ShapeDtypeStruct((NZ - 1, NQ * cap, dim), jnp.bfloat16),
                   jax.ShapeDtypeStruct((2, tok), jnp.int32)),
        in_specs=[any_spec, vmem_spec, any_spec, any_spec, any_spec],
        out_specs=(any_spec, any_spec, vmem_spec),
        scratch_shapes=[
            pltpu.VMEM((NZ, tok, dim), jnp.bfloat16),
            pltpu.VMEM((NQ * cap, dim), jnp.bfloat16),
            pltpu.VMEM((NZ, NQ * cap, dim), jnp.bfloat16),
            pltpu.VMEM((dim, ff), jnp.bfloat16),
            pltpu.VMEM((dim, ff), jnp.bfloat16),
            pltpu.VMEM((ff, dim), jnp.bfloat16),
            pltpu.VMEM((2 * cap, ff), jnp.bfloat16),
            pltpu.VMEM((2 * cap, tok), jnp.bfloat16),
            pltpu.VMEM((NZ, NQ, tok), jnp.float32),
            pltpu.VMEM((NZ, NQ, tok), jnp.float32),
            pltpu.VMEM((NQ, cap), jnp.float32),
            dma(()), dma((3,)), dma((2, NZ - 1, HALVES)), dma((2, NZ - 1, HALVES)),
            dma((NZ,)), dma((NZ,)), dma((NQ,)), dma((NZ, NQ)),
            dma((NZ, NQ)), dma((NZ, NQ)), dma((NZ,)), dma(()),
            dma((NZ, PIECES)), dma((NZ, PIECES)),
        ],
        compiler_params=pltpu.CompilerParams(has_side_effects=True, vmem_limit_bytes=67043328),
        cost_estimate=pl.CostEstimate(flops=flops, bytes_accessed=2 * rows * dim * 4, transcendentals=rows * ff),
    )(hidden_loc, ids_t, w_one, w_three, w_two)


def most_kernel(n, mine_ref, most_ref, theirs, send_sem, recv_sem):
    me = lax.axis_index("ep")

    def copy(slot, target):
        return pltpu.make_async_remote_copy(
            src_ref=mine_ref, dst_ref=theirs.at[slot],
            send_sem=send_sem.at[target], recv_sem=recv_sem.at[slot],
            device_id=(target,), device_id_type=MESH)

    theirs[me] = mine_ref[...]

    @pl.loop(1, n)
    def _(k):
        copy(me, (me + k) % n).start()

    @pl.loop(1, n)
    def _(k):
        copy((me + k) % n, (me + k) % n).wait_recv()

    @pl.loop(1, n)
    def _(k):
        copy(me, (me + k) % n).wait_send()
    most_ref[...] = jnp.max(theirs[...], axis=0)


def most_of_all(mine, n):
    vmem_spec = pl.BlockSpec(memory_space=pltpu.VMEM)
    return pl.pallas_call(
        functools.partial(most_kernel, n),
        out_shape=jax.ShapeDtypeStruct(mine.shape, mine.dtype),
        in_specs=[vmem_spec], out_specs=vmem_spec,
        scratch_shapes=[pltpu.VMEM((n, *mine.shape), mine.dtype),
                        pltpu.SemaphoreType.DMA((n,)), pltpu.SemaphoreType.DMA((n,))],
        compiler_params=pltpu.CompilerParams(has_side_effects=True),
    )(mine)


def route_gates(hidden_loc, w_router, ids_loc):
    logits = jnp.dot(hidden_loc.astype(jnp.float32), w_router, preferred_element_type=jnp.float32)
    prob_vals = jax.nn.softmax(logits, axis=-1)
    exp_iota = lax.broadcasted_iota(jnp.int32, prob_vals.shape, 1)
    p_a = jnp.sum(jnp.where(exp_iota == ids_loc[:, 0:1], prob_vals, 0.0), axis=1, keepdims=True)
    p_b = jnp.sum(jnp.where(exp_iota == ids_loc[:, 1:2], prob_vals, 0.0), axis=1, keepdims=True)
    total = p_a + p_b
    return p_a / total, p_b / total


def solution(mesh):
    n = mesh.shape["ep"]

    def device_body(hidden_loc, w_router, ids_loc, w_one, w_three, w_two):
        tok, dim = hidden_loc.shape
        g_a, g_b = route_gates(hidden_loc, w_router, ids_loc)
        ids_t = ids_loc.T

        def run(limit):
            rows, _, pos = moe_exchange(hidden_loc, ids_t, w_one[0], w_three[0], w_two[0], n, limit)
            both = lax.optimization_barrier(jnp.take(rows, pos.reshape(-1), axis=0, mode="clip"))
            e_a, e_b = both[:tok].astype(jnp.float32), both[tok:].astype(jnp.float32)
            return (g_a * e_a + g_b * e_b).astype(jnp.bfloat16)

        in_plane = ids_t[None] // NQ == jnp.arange(NZ)[:, None, None]
        choices = jnp.max(jnp.sum(in_plane.astype(jnp.float32), axis=(1, 2)))
        most = most_of_all(jnp.full((8, 128), choices, jnp.float32), n)
        limits = (tok * 5 // 8, tok * 11 // 16, tok)
        level = sum((most[0, 0] > limit).astype(jnp.int32) for limit in limits[:-1])
        return lax.switch(level, [functools.partial(run, limit) for limit in limits])

    return jax.shard_map(device_body, mesh=mesh, in_specs=(P("ep", None), P(None, None), P("ep", None), P("ep", None, None), P("ep", None, None), P("ep", None, None)), out_specs=P("ep", None), check_vma=False)
```

```python
import functools

import jax
import jax.numpy as jnp
from jax import lax
from jax.experimental import pallas as pl
from jax.experimental.pallas import tpu as pltpu
from jax.sharding import PartitionSpec as P

MESH = pl.DeviceIdType.MESH
NZ = 4
NQ = 8
HALVES = 2
PIECES = 4


def moe_kernel(limit, cap, hid_hbm, ids_ref, w1_hbm, w3_hbm, w2_hbm, rows_hbm, land_hbm, pos_ref,
               hid, send, recv, w1, w3, w2, act, sel, rank, rank_in, slots,
               own_sem, w_sem, z_send, z_recv, r_send, r_recv,
               p_send, p_recv, l_send, l_recv, loc_sem, stage_sem, b_send, b_recv):
    me = lax.axis_index("ep")
    z = me // NQ
    q = me % NQ
    mirror = z // 2
    zz = z + mirror * (3 - 2 * z)
    tok = hid_hbm.shape[0]
    dim = hid_hbm.shape[1]
    ff = w1.shape[1]
    piece = limit // PIECES
    back_base = NQ * cap
    half_tok = tok // HALVES
    pair = 2 * cap
    nt = min(256, dim)
    ft = min(256, ff)

    def block_of(step):
        near = (0, 1, 2, 3)[step]
        inner = (1, 2, 0, 3)[step]
        pick = near + zz * (inner - near)
        return pick + mirror * (3 - 2 * pick)

    def partner(c):
        px, py = (q // 2) % 2, q // 4
        return 2 * (py + (c // 2) * (1 - 2 * py)) + px + (c % 2) * (1 - 2 * px)

    def half(ref, h):
        return ref.at[pl.ds(h * half_tok, half_tok)]

    def z_copy(direction, hop, h, block, src=None):
        target = me + (NQ if direction == 0 else -NQ)
        return pltpu.make_async_remote_copy(
            src_ref=half(hid.at[block] if src is None else src, h),
            dst_ref=half(hid.at[block], h),
            send_sem=z_send.at[direction, hop - 1, h],
            recv_sem=z_recv.at[direction, hop - 1, h],
            device_id=(target,), device_id_type=MESH)

    def rank_copy(plane):
        return pltpu.make_async_remote_copy(
            src_ref=rank.at[plane], dst_ref=rank_in.at[z],
            send_sem=r_send.at[plane], recv_sem=r_recv.at[z],
            device_id=(plane * NQ + q,), device_id_type=MESH)

    def plane_copy(step, peer):
        return pltpu.make_async_remote_copy(
            src_ref=send.at[pl.ds(peer * cap, cap)],
            dst_ref=recv.at[step, pl.ds(q * cap, cap)],
            send_sem=p_send.at[peer], recv_sem=p_recv.at[step, q],
            device_id=(z * NQ + peer,), device_id_type=MESH)

    def plane_arrival(step, peer):
        return pltpu.make_async_remote_copy(
            src_ref=send.at[pl.ds(peer * cap, cap)],
            dst_ref=recv.at[step, pl.ds(peer * cap, cap)],
            send_sem=p_send.at[peer], recv_sem=p_recv.at[step, peer],
            device_id=(z * NQ + peer,), device_id_type=MESH)

    def landing(step, peer):
        home = rows_hbm if step == 0 else land_hbm.at[step - 1]
        return home.at[pl.ds(peer * cap, cap)]

    def land_copy(step, peer):
        return pltpu.make_async_remote_copy(
            src_ref=recv.at[step, pl.ds(peer * cap, cap)], dst_ref=landing(step, q),
            send_sem=l_send.at[step, peer], recv_sem=l_recv.at[step, q],
            device_id=(z * NQ + peer,), device_id_type=MESH)

    def land_arrival(step, peer):
        return pltpu.make_async_remote_copy(
            src_ref=recv.at[step, pl.ds(peer * cap, cap)], dst_ref=landing(step, peer),
            send_sem=l_send.at[step, peer], recv_sem=l_recv.at[step, peer],
            device_id=(z * NQ + peer,), device_id_type=MESH)

    def land_own(step):
        return pltpu.make_async_copy(recv.at[step, pl.ds(q * cap, cap)], landing(step, q), loc_sem.at[step])

    def back_copy(step, g, plane, owner):
        return pltpu.make_async_remote_copy(
            src_ref=recv.at[step, pl.ds(g * piece, piece)],
            dst_ref=rows_hbm.at[pl.ds(back_base + plane * limit + g * piece, piece)],
            send_sem=b_send.at[step, g], recv_sem=b_recv.at[plane, g],
            device_id=(owner * NQ + q,), device_id_type=MESH)

    own_load = pltpu.make_async_copy(hid_hbm, hid.at[z], own_sem)
    for h in range(HALVES):
        @pl.when(z < NZ - 1)
        def _():
            z_copy(0, 1, h, z, hid_hbm).start()

        @pl.when(z > 0)
        def _():
            z_copy(1, 1, h, z, hid_hbm).start()
    own_load.start()
    w_loads = [pltpu.make_async_copy(src, dst, w_sem.at[k])
               for k, (src, dst) in enumerate(((w1_hbm, w1), (w3_hbm, w3), (w2_hbm, w2)))]
    for load in w_loads:
        load.start()

    n_exp = NZ * NQ
    lanes = min(256, tok)
    exp_iota = lax.broadcasted_iota(jnp.int32, (n_exp, lanes), 0)
    row_iota = lax.broadcasted_iota(jnp.int32, (lanes, lanes), 0)
    col_iota = lax.broadcasted_iota(jnp.int32, (lanes, lanes), 1)
    below = (row_iota < col_iota).astype(jnp.float32).astype(jnp.bfloat16)
    carry = jnp.zeros((n_exp, 1), jnp.float32)
    for k in range(tok // lanes):
        span = pl.ds(k * lanes, lanes)
        first = ids_ref[pl.ds(0, 1), span] == exp_iota
        second = ids_ref[pl.ds(1, 1), span] == exp_iota
        chosen = jnp.where(first, 1.0, 0.0) + jnp.where(second, 1.0, 0.0)
        count = jnp.dot(chosen.astype(jnp.bfloat16), below, preferred_element_type=jnp.float32) + carry
        carry = carry + jnp.sum(chosen, axis=1, keepdims=True)
        marked = jnp.where(chosen > 0.5, count, -1.0)
        for plane in range(NZ):
            rank[plane, :, span] = marked[plane * NQ:(plane + 1) * NQ]
    for plane in range(NZ):
        @pl.when(z != plane)
        def _():
            rank_copy(plane).start()

        @pl.when(z == plane)
        def _():
            rank_in[plane] = rank[plane]

    base = []
    for plane in range(NZ):
        run = jnp.zeros((1, 1), jnp.float32)
        for e in range(NQ):
            there = run + (back_base + plane * limit)
            base.append(jnp.where(z == plane, float(e * cap), there))
            run = run + carry[plane * NQ + e:plane * NQ + e + 1, :]
    base = jnp.concatenate(base, axis=0)
    for k in range(tok // lanes):
        span = pl.ds(k * lanes, lanes)
        place = jnp.concatenate([rank[plane, :, span] for plane in range(NZ)], axis=0) + base
        for j in range(2):
            hit = ids_ref[pl.ds(j, 1), span] == exp_iota
            pos_ref[pl.ds(j, 1), span] = jnp.sum(
                jnp.where(hit, place, 0.0), axis=0, keepdims=True).astype(jnp.int32)

    def relay(hop, h):
        @pl.when(z >= hop)
        def _():
            z_copy(0, hop, h, z - hop).wait_recv()

        @pl.when(jnp.logical_and(z >= hop, z < NZ - 1))
        def _():
            z_copy(0, hop + 1, h, z - hop).start()

        @pl.when(z + hop < NZ)
        def _():
            z_copy(1, hop, h, z + hop).wait_recv()

        @pl.when(jnp.logical_and(z + hop < NZ, z > 0))
        def _():
            z_copy(1, hop + 1, h, z + hop).start()

    def select(step):
        block = block_of(step)
        if step > 0:
            pltpu.make_async_remote_copy(
                src_ref=rank.at[0], dst_ref=rank_in.at[block],
                send_sem=r_send.at[block], recv_sem=r_recv.at[block],
                device_id=(block * NQ + q,), device_id_type=MESH).wait_recv()
        slot_iota = lax.broadcasted_iota(jnp.int32, (cap, tok), 0).astype(jnp.float32)

        @pl.loop(0, NQ // 2)
        def _(k):
            p = partner((k + 1) % (NQ // 2))
            for j in range(2):
                peer = 2 * p + j
                if step > 0:
                    @pl.when(peer != q)
                    def _():
                        plane_copy(step - 1, peer).wait_send()
                row = rank_in[block, pl.ds(peer, 1), :]
                sel[pl.ds(j * cap, cap), :] = jnp.where(slot_iota == row, 1.0, 0.0).astype(jnp.bfloat16)

            @pl.loop(0, dim // nt)
            def _(n):
                cols = pl.ds(pl.multiple_of(n * nt, nt), nt)
                send[pl.ds(p * pair, pair), cols] = jnp.dot(
                    sel[...], hid[block, :, cols], preferred_element_type=jnp.float32).astype(jnp.bfloat16)

            for j in range(2):
                peer = 2 * p + j

                @pl.when(peer != q)
                def _():
                    plane_copy(step, peer).start()

                @pl.when(peer == q)
                def _():
                    recv[step, pl.ds(peer * cap, cap), :] = send[pl.ds(peer * cap, cap), :]

    def experts(step):
        @pl.loop(0, NQ // 2)
        def _(k):
            p = partner(k)
            for j in range(2):
                peer = 2 * p + j

                @pl.when(peer != q)
                def _():
                    plane_arrival(step, peer).wait_recv()
            rows = pl.ds(p * pair, pair)

            @pl.loop(0, ff // ft)
            def _(f):
                cols = pl.ds(pl.multiple_of(f * ft, ft), ft)
                x = recv[step, rows, :]
                u = jnp.dot(x, w1[:, cols], preferred_element_type=jnp.float32)
                v = jnp.dot(x, w3[:, cols], preferred_element_type=jnp.float32)
                act[:, cols] = (jax.nn.silu(u) * v).astype(jnp.bfloat16)

            @pl.loop(0, dim // nt)
            def _(n):
                cols = pl.ds(pl.multiple_of(n * nt, nt), nt)
                recv[step, rows, cols] = jnp.dot(
                    act[...], w2[:, cols], preferred_element_type=jnp.float32).astype(jnp.bfloat16)

            for j in range(2):
                peer = 2 * p + j

                @pl.when(peer != q)
                def _():
                    land_copy(step, peer).start()

                @pl.when(peer == q)
                def _():
                    land_own(step).start()

    def landed(step):
        @pl.loop(0, NQ)
        def _(peer):
            @pl.when(peer != q)
            def _():
                land_arrival(step, peer).wait_recv()
                land_copy(step, peer).wait_send()
        land_own(step).wait()

    def give_back(step):
        block = block_of(step)
        for h in range(HALVES):
            @pl.when(jnp.logical_and(block < z, z < NZ - 1))
            def _():
                z_copy(0, z - block + 1, h, block).wait_send()

            @pl.when(jnp.logical_and(block > z, z > 0))
            def _():
                z_copy(1, block - z + 1, h, block).wait_send()
        landed(step)
        stage = pltpu.make_async_copy(land_hbm.at[step - 1], hid.at[block], stage_sem)
        stage.start()
        slot_iota = lax.broadcasted_iota(jnp.int32, (1, cap), 1).astype(jnp.float32)
        run = jnp.zeros((1, 1), jnp.float32)
        for e in range(NQ):
            taken = jnp.sum(jnp.where(rank_in[block, pl.ds(e, 1), :] >= 0.0, 1.0, 0.0), axis=1, keepdims=True)
            slots[pl.ds(e, 1), :] = jnp.where(slot_iota < taken, slot_iota + run, -1.0)
            run = run + taken
        stage.wait()

        @pl.loop(0, PIECES)
        def _(g):
            place = (lax.broadcasted_iota(jnp.int32, (piece, cap), 0) + g * piece).astype(jnp.float32)
            for e in range(NQ):
                sel[pl.ds(0, piece), pl.ds(e * cap, cap)] = jnp.where(
                    place == slots[pl.ds(e, 1), :], 1.0, 0.0).astype(jnp.bfloat16)

            @pl.loop(0, dim // nt)
            def _(n):
                cols = pl.ds(pl.multiple_of(n * nt, nt), nt)
                recv[step, pl.ds(g * piece, piece), cols] = jnp.dot(
                    sel[pl.ds(0, piece), :], hid[block, :, cols],
                    preferred_element_type=jnp.float32).astype(jnp.bfloat16)
            back_copy(step, g, z, block).start()

    own_load.wait()
    select(0)
    relay(1, 0)
    relay(1, 1)
    select(1)
    for load in w_loads:
        load.wait()
    experts(0)
    relay(2, 0)
    experts(1)
    relay(2, 1)
    select(2)
    give_back(1)
    experts(2)
    for h in range(HALVES):
        @pl.when(z >= 3)
        def _():
            z_copy(0, 3, h, z - 3).wait_recv()

        @pl.when(z + 3 < NZ)
        def _():
            z_copy(1, 3, h, z + 3).wait_recv()
    select(3)
    give_back(2)
    experts(3)
    give_back(3)

    for h in range(HALVES):
        @pl.when(z < NZ - 1)
        def _():
            z_copy(0, 1, h, z).wait_send()

        @pl.when(z > 0)
        def _():
            z_copy(1, 1, h, z).wait_send()
    for plane in range(NZ):
        @pl.when(z != plane)
        def _():
            rank_copy(plane).wait_send()

    @pl.loop(0, NQ)
    def _(peer):
        @pl.when(peer != q)
        def _():
            plane_copy(NZ - 1, peer).wait_send()
    landed(0)

    @pl.loop(0, PIECES)
    def _(g):
        for step in range(1, NZ):
            back_copy(step, g, z, block_of(step)).wait_send()
            back_copy(step, g, block_of(step), block_of(step)).wait_recv()


def moe_exchange(hidden_loc, ids_t, w_one, w_three, w_two, n, limit):
    tok, dim = hidden_loc.shape
    ff = w_one.shape[1]
    cap = 4 * tok // n
    any_spec = pl.BlockSpec(memory_space=pl.ANY)
    vmem_spec = pl.BlockSpec(memory_space=pltpu.VMEM)
    dma = pltpu.SemaphoreType.DMA
    rows = n * cap
    flops = 2 * rows * (3 * dim * ff + 2 * tok * dim)
    return pl.pallas_call(
        functools.partial(moe_kernel, limit, cap),
        out_shape=(jax.ShapeDtypeStruct((NQ * cap + NZ * limit, dim), jnp.bfloat16),
                   jax.ShapeDtypeStruct((NZ - 1, NQ * cap, dim), jnp.bfloat16),
                   jax.ShapeDtypeStruct((2, tok), jnp.int32)),
        in_specs=[any_spec, vmem_spec, any_spec, any_spec, any_spec],
        out_specs=(any_spec, any_spec, vmem_spec),
        scratch_shapes=[
            pltpu.VMEM((NZ, tok, dim), jnp.bfloat16),
            pltpu.VMEM((NQ * cap, dim), jnp.bfloat16),
            pltpu.VMEM((NZ, NQ * cap, dim), jnp.bfloat16),
            pltpu.VMEM((dim, ff), jnp.bfloat16),
            pltpu.VMEM((dim, ff), jnp.bfloat16),
            pltpu.VMEM((ff, dim), jnp.bfloat16),
            pltpu.VMEM((2 * cap, ff), jnp.bfloat16),
            pltpu.VMEM((2 * cap, tok), jnp.bfloat16),
            pltpu.VMEM((NZ, NQ, tok), jnp.float32),
            pltpu.VMEM((NZ, NQ, tok), jnp.float32),
            pltpu.VMEM((NQ, cap), jnp.float32),
            dma(()), dma((3,)), dma((2, NZ - 1, HALVES)), dma((2, NZ - 1, HALVES)),
            dma((NZ,)), dma((NZ,)), dma((NQ,)), dma((NZ, NQ)),
            dma((NZ, NQ)), dma((NZ, NQ)), dma((NZ,)), dma(()),
            dma((NZ, PIECES)), dma((NZ, PIECES)),
        ],
        compiler_params=pltpu.CompilerParams(has_side_effects=True, vmem_limit_bytes=67043328),
        cost_estimate=pl.CostEstimate(flops=flops, bytes_accessed=2 * rows * dim * 4, transcendentals=rows * ff),
    )(hidden_loc, ids_t, w_one, w_three, w_two)


def most_kernel(n, mine_ref, most_ref, theirs, send_sem, recv_sem):
    me = lax.axis_index("ep")

    def copy(slot, target):
        return pltpu.make_async_remote_copy(
            src_ref=mine_ref, dst_ref=theirs.at[slot],
            send_sem=send_sem.at[target], recv_sem=recv_sem.at[slot],
            device_id=(target,), device_id_type=MESH)

    theirs[me] = mine_ref[...]

    @pl.loop(1, n)
    def _(k):
        copy(me, (me + k) % n).start()

    @pl.loop(1, n)
    def _(k):
        copy((me + k) % n, (me + k) % n).wait_recv()

    @pl.loop(1, n)
    def _(k):
        copy(me, (me + k) % n).wait_send()
    most_ref[...] = jnp.max(theirs[...], axis=0)


def most_of_all(mine, n):
    vmem_spec = pl.BlockSpec(memory_space=pltpu.VMEM)
    return pl.pallas_call(
        functools.partial(most_kernel, n),
        out_shape=jax.ShapeDtypeStruct(mine.shape, mine.dtype),
        in_specs=[vmem_spec], out_specs=vmem_spec,
        scratch_shapes=[pltpu.VMEM((n, *mine.shape), mine.dtype),
                        pltpu.SemaphoreType.DMA((n,)), pltpu.SemaphoreType.DMA((n,))],
        compiler_params=pltpu.CompilerParams(has_side_effects=True),
    )(mine)


def route_gates(hidden_loc, w_router, ids_loc):
    logits = jnp.dot(hidden_loc.astype(jnp.float32), w_router, preferred_element_type=jnp.float32)
    prob_vals = jax.nn.softmax(logits, axis=-1)
    exp_iota = lax.broadcasted_iota(jnp.int32, prob_vals.shape, 1)
    p_a = jnp.sum(jnp.where(exp_iota == ids_loc[:, 0:1], prob_vals, 0.0), axis=1, keepdims=True)
    p_b = jnp.sum(jnp.where(exp_iota == ids_loc[:, 1:2], prob_vals, 0.0), axis=1, keepdims=True)
    total = p_a + p_b
    return p_a / total, p_b / total


def solution(mesh):
    n = mesh.shape["ep"]

    def device_body(hidden_loc, w_router, ids_loc, w_one, w_three, w_two):
        tok, dim = hidden_loc.shape
        g_a, g_b = route_gates(hidden_loc, w_router, ids_loc)
        ids_t = ids_loc.T

        def run(limit):
            rows, _, pos = moe_exchange(hidden_loc, ids_t, w_one[0], w_three[0], w_two[0], n, limit)
            both = lax.optimization_barrier(jnp.take(rows, pos.reshape(-1), axis=0, mode="clip"))
            e_a, e_b = both[:tok].astype(jnp.float32), both[tok:].astype(jnp.float32)
            return (g_a * e_a + g_b * e_b).astype(jnp.bfloat16)

        in_plane = ids_t[None] // NQ == jnp.arange(NZ)[:, None, None]
        choices = jnp.max(jnp.sum(in_plane.astype(jnp.float32), axis=(1, 2)))
        most = most_of_all(jnp.full((8, 128), choices, jnp.float32), n)
        limits = (tok * 19 // 32, tok * 11 // 16, tok)
        level = sum((most[0, 0] > limit).astype(jnp.int32) for limit in limits[:-1])
        return lax.switch(level, [functools.partial(run, limit) for limit in limits])

    return jax.shard_map(device_body, mesh=mesh, in_specs=(P("ep", None), P(None, None), P("ep", None), P("ep", None, None), P("ep", None, None), P("ep", None, None)), out_specs=P("ep", None), check_vma=False)
```
